32 devices in a mesh: data: 4 (over y, z), seq: 8 (over x, core).
Axes of the slice: x: 4, y: 2, z: 2, core: 2. Of those that a mesh axis runs over, the one named last changes fastest.
The devices are a block of a 4x4x8 slice.
Arguments:
- x: bfloat16 [16384, 5120], P(('data', 'seq')), parts along dimension 0
- g: float32 [5120], replicated
- wqkv: bfloat16 [5120, 3, 40, 128], replicated
- wo: bfloat16 [40, 128, 5120], replicated
Outputs:
- output: bfloat16 [16384, 5120], P(('data', 'seq')), parts along dimension 0
There are 4 independent parts. The reference program is written for one: setup_inputs(seed, part) draws one part's arguments, and reference() takes and returns one part's arrays. A program takes and returns all parts, laid end to end along the dimension named above; an argument that names none is the same for every part.
All inputs are finite; a program needn't handle non-finite values.
Results may differ from the reference program's by a relative error of at most 0.00308505.
Values are sent between devices in bfloat16 or wider.
A program may use at most 768 MiB of HBM per device.

```python
import jax
import jax.numpy as jnp
from jax import lax

S = 4096
D = 5120
HEADS = 40
HEAD = 128


def setup_inputs(seed: int = 0, part: int = 0) -> dict:
    k_shared, k_part = jax.random.split(jax.random.PRNGKey(seed))
    kx, kf, ku = jax.random.split(jax.random.fold_in(k_part, part), 3)
    kg, kq, ko = jax.random.split(k_shared, 3)
    r = jnp.arange(S, dtype=jnp.float32)[:, None] / S
    freq = jnp.array([0.5, 1.0, 1.5, 2.5], jnp.float32)
    phase = jax.random.uniform(kf, (4,), jnp.float32, 0.0, 2.0 * jnp.pi)
    waves = jnp.sin(2.0 * jnp.pi * r * freq + phase)
    u = jax.random.normal(ku, (4, D), jnp.float32)
    x = 0.25 * jax.random.normal(kx, (S, D), jnp.float32) + 0.35 * (waves @ u)
    g = 1.0 + 0.2 * jax.random.normal(kg, (D,), jnp.float32)
    wqkv = jax.random.normal(kq, (D, 3, HEADS, HEAD), jnp.float32) * D ** -0.5
    wo = jax.random.normal(ko, (HEADS, HEAD, D), jnp.float32) * (HEADS * HEAD) ** -0.5
    return {"x": x.astype(jnp.bfloat16), "g": g, "wqkv": wqkv.astype(jnp.bfloat16), "wo": wo.astype(jnp.bfloat16)}


def _rope(x, pos):
    half = HEAD // 2
    inv = 10000.0 ** (-jnp.arange(half, dtype=jnp.float32) * 2.0 / HEAD)
    ang = pos[:, None] * inv[None, :]
    cos = jnp.cos(ang)[:, None, :]
    sin = jnp.sin(ang)[:, None, :]
    x1, x2 = x[..., :half], x[..., half:]
    return jnp.concatenate([x1 * cos - x2 * sin, x2 * cos + x1 * sin], axis=-1)


def reference(x, g, wqkv, wo):
    xf = x.astype(jnp.float32)
    xn = (xf * lax.rsqrt(jnp.mean(xf * xf, axis=-1, keepdims=True) + 1e-5) * g).astype(jnp.bfloat16)
    qkv = jnp.dot(xn, wqkv.reshape(D, 3 * HEADS * HEAD), preferred_element_type=jnp.float32).reshape(S, 3, HEADS, HEAD)
    pos = jnp.arange(S, dtype=jnp.float32)
    q = _rope(qkv[:, 0], pos).astype(jnp.bfloat16)
    k = _rope(qkv[:, 1], pos).astype(jnp.bfloat16)
    v = qkv[:, 2].astype(jnp.bfloat16)
    qb = min(S, 512)
    nq = S // qb
    scale = HEAD ** -0.5

    def one_head(args):
        qh, kh, vh = args

        def one_block(a):
            qblk, i = a
            sc = jnp.dot(qblk, kh.T, preferred_element_type=jnp.float32) * scale
            mask = (i * qb + jnp.arange(qb))[:, None] >= jnp.arange(S)[None, :]
            sc = jnp.where(mask, sc, -jnp.inf)
            pr = jax.nn.softmax(sc, axis=-1).astype(jnp.bfloat16)
            return jnp.dot(pr, vh, preferred_element_type=jnp.float32).astype(jnp.bfloat16)

        o = lax.map(one_block, (qh.reshape(nq, qb, HEAD), jnp.arange(nq)))
        return o.reshape(S, HEAD)

    o = lax.map(one_head, (q.transpose(1, 0, 2), k.transpose(1, 0, 2), v.transpose(1, 0, 2)))
    o = o.transpose(1, 0, 2).reshape(S, HEADS * HEAD)
    y = xf + jnp.dot(o, wo.reshape(HEADS * HEAD, D), preferred_element_type=jnp.float32)
    return y.astype(jnp.bfloat16)
```

```python
import functools

import jax
import jax.numpy as jnp
from jax import lax
from jax.experimental import pallas as pl
from jax.experimental.pallas import tpu as pltpu
from jax.sharding import PartitionSpec as P

LOG2E = 1.4426950408889634
VMEM_LIMIT = 60 * 1024 * 1024


def _qkv_kernel(nx, nrope, *refs):
    xs, w_ref, cos_ref, sin_ref, out_ref = refs[:nx], *refs[nx:]
    n = pl.program_id(0)
    nh, _, rb, dh = out_ref.shape
    steps = pl.num_programs(0)
    w = jnp.concatenate([w_ref[h] for h in range(nh)], axis=1)

    @pl.when(n < nrope)
    def _():
        for i in range(nx):
            acc = jnp.dot(xs[i][...], w, preferred_element_type=jnp.float32)
            for h in range(nh):
                a = acc[:, h * dh:(h + 1) * dh]
                rot = pltpu.roll(a, dh // 2, 1)
                out_ref[h, i] = (a * cos_ref[i] + rot * sin_ref[i]).astype(out_ref.dtype)

    @pl.when(jnp.logical_and(n >= nrope, n < steps - 1))
    def _():
        for i in range(nx):
            acc = jnp.dot(xs[i][...], w, preferred_element_type=jnp.float32)
            for h in range(nh):
                out_ref[h, i] = acc[:, h * dh:(h + 1) * dh].astype(out_ref.dtype)

    @pl.when(n == steps - 1)
    def _():
        for i in range(nx):
            out_ref[0, i] = jnp.dot(xs[i][...], w_ref[0], preferred_element_type=jnp.float32).astype(out_ref.dtype)


def _qkv(xs, w, cos, sin):
    nx = len(xs)
    rb, d = xs[0].shape
    nh, _, dh = w.shape
    assert nh % 2 == 1
    return pl.pallas_call(
        functools.partial(_qkv_kernel, nx, nh // 3),
        out_shape=jax.ShapeDtypeStruct((nh, nx, rb, dh), xs[0].dtype),
        grid=(pl.cdiv(nh, 2),),
        in_specs=[pl.BlockSpec((rb, d), lambda n: (0, 0), pipeline_mode=pl.Buffered(1)) for _ in xs] + [
            pl.BlockSpec((2, d, dh), lambda n: (n, 0, 0)),
            pl.BlockSpec((nx, rb, dh), lambda n: (0, 0, 0), pipeline_mode=pl.Buffered(1)),
            pl.BlockSpec((nx, rb, dh), lambda n: (0, 0, 0), pipeline_mode=pl.Buffered(1))],
        out_specs=pl.BlockSpec((2, nx, rb, dh), lambda n: (n, 0, 0, 0)),
        compiler_params=pltpu.CompilerParams(vmem_limit_bytes=VMEM_LIMIT),
        cost_estimate=pl.CostEstimate(flops=2 * nx * rb * d * nh * dh, transcendentals=0,
                                      bytes_accessed=2 * (nx * rb * d + d * nh * dh + nx * rb * nh * dh)),
        name="qkv",
    )(*xs, w, cos, sin)


def _attn_body(q_ref, k_ref, v_ref, put, sa_ref, sb_ref, ma_ref, mb_ref, l_ref, acc_ref):
    nb, _, b = sa_ref.shape
    dh = acc_ref.shape[1]
    c = dh ** -0.5 * LOG2E
    lanes = [slice(t * dh, (t + 1) * dh) for t in range(b // dh)]
    sc, mx = (sa_ref, sb_ref), (ma_ref, mb_ref)

    def rows(ref, i):
        return ref[pl.ds(pl.multiple_of(i * b, b), b), :]

    def scores(i, j):
        return lax.dot_general(rows(q_ref, i), rows(k_ref, j), (((1,), (1,)), ((), ())),
                               preferred_element_type=jnp.float32)

    def lanemax(m, x):
        for t in lanes:
            m = jnp.maximum(m, x[:, t])
        return m

    def pass1(i, j, slot):
        x = scores(i, j)
        sc[slot][j] = x
        mx[slot][...] = lanemax(mx[slot][...], x)

    def pass1_diag(i, slot):
        x = scores(i, i)
        x = jnp.where(lax.broadcasted_iota(jnp.int32, x.shape, 0) >= lax.broadcasted_iota(jnp.int32, x.shape, 1),
                      x, -jnp.inf)
        sc[slot][i] = x
        m = lanemax(mx[slot][...], x)
        mx[slot][...] = jnp.broadcast_to(jnp.max(m, axis=1, keepdims=True), m.shape)

    def pass2(j, slot):
        m, l, ps = mx[slot][...], l_ref[...], []
        for t in lanes:
            e = jnp.exp2((sc[slot][j, :, t] - m) * c)
            l = l + e
            ps.append(e.astype(v_ref.dtype))
        l_ref[...] = l
        acc_ref[...] += jnp.dot(jnp.concatenate(ps, axis=1), rows(v_ref, j), preferred_element_type=jnp.float32)

    def clear_max(slot):
        mx[slot][...] = jnp.full(mx[slot].shape, -jnp.inf, jnp.float32)

    def block(i, cur):
        l_ref[...] = jnp.zeros_like(l_ref)
        acc_ref[...] = jnp.zeros_like(acc_ref)
        last = isinstance(i, int) and i == nb - 1
        if not last:
            clear_max(1 - cur)

        def inner(j, _):
            if not last:
                pass1(i + 1, j, 1 - cur)
            pass2(j, cur)
            return 0

        lax.fori_loop(0, i + 1, inner, 0)
        if not last:
            pass1_diag(i + 1, 1 - cur)
        put(i, (acc_ref[...] / jnp.sum(l_ref[...], axis=1, keepdims=True)).astype(v_ref.dtype))

    clear_max(0)
    pass1_diag(0, 0)
    for i in range(nb):
        block(i, i % 2)


def _attn_kernel(h, hl, n, idx_ref, *refs):
    qkv, (o_ref, q_ref, k_ref, v_ref, sem), scratch = refs[:n], refs[n:n + 5], refs[n + 5:]
    rb = qkv[0].shape[2]
    copies, done = [], 0
    for a in qkv:
        for i in range(a.shape[1]):
            at = pl.ds(pl.multiple_of(idx_ref[done + i] * rb, rb), rb)
            for j, dst in enumerate((q_ref, k_ref, v_ref)):
                copies.append(pltpu.make_async_copy(a.at[j * hl + h, i], dst.at[at, :], sem.at[len(copies)]))
        done += a.shape[1]
    for cp in copies:
        cp.start()
    for cp in copies:
        cp.wait()
    t = o_ref.shape[1]

    def put(i, o):
        k = o.shape[0] // t
        for u in range(k):
            o_ref[i * k + u] = o[u * t:(u + 1) * t]

    _attn_body(q_ref, k_ref, v_ref, put, *scratch)


def _attn(qkv, idx, h, p, b=1024):
    n = len(qkv)
    nh, _, rb, dh = qkv[0].shape
    nx = sum(a.shape[1] for a in qkv)
    s = nx * rb
    f32 = jnp.float32
    return pl.pallas_call(
        functools.partial(_attn_kernel, h, nh // 3, n),
        out_shape=jax.ShapeDtypeStruct((p, s // p, dh), qkv[0].dtype),
        grid_spec=pltpu.PrefetchScalarGridSpec(
            num_scalar_prefetch=1,
            grid=(1,),
            in_specs=[pl.BlockSpec(memory_space=pl.ANY)] * n,
            out_specs=pl.BlockSpec((p, s // p, dh), lambda i, idx: (0, 0, 0), pipeline_mode=pl.Buffered(1)),
            scratch_shapes=[pltpu.VMEM((s, dh), qkv[0].dtype)] * 3 + [pltpu.SemaphoreType.DMA((3 * nx,))] + [
                pltpu.VMEM((s // b, b, b), f32), pltpu.VMEM((s // b, b, b), f32), pltpu.VMEM((b, dh), f32),
                pltpu.VMEM((b, dh), f32), pltpu.VMEM((b, dh), f32), pltpu.VMEM((b, dh), f32)]),
        compiler_params=pltpu.CompilerParams(vmem_limit_bytes=VMEM_LIMIT),
        cost_estimate=pl.CostEstimate(flops=2 * 2 * s * s * dh, transcendentals=s * s // 2,
                                      bytes_accessed=2 * 4 * s * dh),
        name="attn",
    )(idx, *qkv)


def _out_kernel(nc, *refs):
    os, (w_ref, x_ref, y_ref) = refs[:nc], refs[nc:]
    acc = x_ref[...].astype(jnp.float32)
    p, _, dh, cols = w_ref.shape
    for c in range(nc):
        o = jnp.concatenate([os[c][s] for s in range(p)], axis=1)
        acc += jnp.dot(o, w_ref[:, c].reshape(p * dh, cols), preferred_element_type=jnp.float32)
    y_ref[...] = acc.astype(y_ref.dtype)


def _out(os, wo, x, cols=512):
    nc = len(os)
    p, t, dh = os[0].shape
    d = x.shape[1]
    return pl.pallas_call(
        functools.partial(_out_kernel, nc),
        out_shape=jax.ShapeDtypeStruct(x.shape, x.dtype),
        grid=(d // cols,),
        in_specs=[pl.BlockSpec((p, t, dh), lambda n: (0, 0, 0), pipeline_mode=pl.Buffered(1)) for _ in os] + [
            pl.BlockSpec((p, nc, dh, cols), lambda n: (0, 0, 0, n)),
            pl.BlockSpec((t, cols), lambda n: (0, n))],
        out_specs=pl.BlockSpec((t, cols), lambda n: (0, n)),
        compiler_params=pltpu.CompilerParams(vmem_limit_bytes=VMEM_LIMIT),
        cost_estimate=pl.CostEstimate(flops=2 * t * d * p * nc * dh, transcendentals=0,
                                      bytes_accessed=2 * (p * nc * dh * d + 3 * t * d)),
        name="outproj",
    )(*os, wo.reshape(p, nc, dh, d), x)


def _shift(a, p, k):
    return lax.ppermute(a, "seq", [(i, (i + k) % p) for i in range(p)])


def _partner(a, p):
    return lax.ppermute(a, "seq", [(i, i ^ 1) for i in range(p)])


def solution(mesh):
    p = mesh.shape["seq"]
    rows = P(("data", "seq"), None)

    def local(x, g, wqkv, wo):
        t, d = x.shape
        _, _, h, dh = wqkv.shape
        hl = h // p
        me = lax.axis_index("seq")
        rb = t // 2

        def norm(x):
            xf = x.astype(jnp.float32)
            return (xf * lax.rsqrt(jnp.mean(xf * xf, axis=-1, keepdims=True) + 1e-5) * g).astype(jnp.bfloat16)

        xa, xb = norm(x[:rb]), norm(x[rb:])
        left_a, right_b = _shift(xa, p, 2), _shift(xb, p, -2)
        left_b, right_a = _shift(xb, p, 2), _shift(xa, p, -2)

        w = lax.dynamic_slice_in_dim(wqkv, hl * me, hl, 2).transpose(1, 2, 0, 3).reshape(3 * hl, d, dh)
        half = dh // 2
        inv = 10000.0 ** (-jnp.arange(half, dtype=jnp.float32) * 2.0 / dh)

        def tables(group):
            idx = jnp.stack([2 * ((m + k + p) % p) + i for m in (me, me ^ 1) for k, i in group])
            ang = (idx[:, None] * rb + jnp.arange(rb)).astype(jnp.float32)[:, :, None] * inv
            cos, sin = jnp.cos(ang), jnp.sin(ang)
            return idx, jnp.concatenate([cos, cos], 2), jnp.concatenate([-sin, sin], 2)

        def with_mates(*xs):
            return list(xs) + [_partner(a, p) for a in xs]

        i0, *cs0 = tables([(0, 0), (0, 1)])
        i1, *cs1 = tables([(-2, 0), (2, 1), (-2, 1), (2, 0)])
        i2, *cs2 = tables([(4, 0), (4, 1)])
        qkv = [_qkv(with_mates(xa, xb), w, *cs0)]
        left_a, right_b, left_b, right_a, cs1, cs2, qkv[0] = lax.optimization_barrier(
            (left_a, right_b, left_b, right_a, cs1, cs2, qkv[0]))
        opp_a, opp_b = _shift(left_a, p, 2), _shift(right_b, p, -2)
        qkv.append(_qkv(with_mates(left_a, right_b, left_b, right_a), w, *cs1))
        qkv.append(_qkv(with_mates(opp_a, opp_b), w, *cs2))
        idx = jnp.concatenate([i0, i1, i2]).astype(jnp.int32)

        os = [lax.all_to_all(_attn(qkv, idx, c, p), "seq", 0, 0) for c in range(hl)]
        return _out(os, wo, x)

    return jax.shard_map(local, mesh=mesh,
                         in_specs=(rows, P(None), P(None, None, None, None), P(None, None, None)),
                         out_specs=rows, check_vma=False)
```

```python
import functools

import jax
import jax.numpy as jnp
from jax import lax
from jax.experimental import pallas as pl
from jax.experimental.pallas import tpu as pltpu
from jax.sharding import PartitionSpec as P

LOG2E = 1.4426950408889634
VMEM_LIMIT = 60 * 1024 * 1024


def _qkv_kernel(nx, *refs):
    xs, w_ref, cos_ref, sin_ref, out_ref = refs[:nx], *refs[nx:]
    n, steps = pl.program_id(0), pl.num_programs(0)
    nh, _, rb, dh = out_ref.shape

    @pl.when(n < steps - 1)
    def _():
        w = jnp.concatenate([w_ref[h] for h in range(nh)], axis=1)
        for i in range(nx):
            acc = jnp.dot(xs[i][...], w, preferred_element_type=jnp.float32)
            for h in range(nh):
                a = acc[:, h * dh:(h + 1) * dh]
                rot = pltpu.roll(a, dh // 2, 1)
                out_ref[h, i] = (a * cos_ref[0, i] + rot * sin_ref[0, i]).astype(out_ref.dtype)

    @pl.when(n == steps - 1)
    def _():
        for i in range(nx):
            out_ref[0, i] = jnp.dot(xs[i][...], w_ref[0], preferred_element_type=jnp.float32).astype(out_ref.dtype)


def _qkv(xs, w, cos, sin):
    nx = len(xs)
    rb, d = xs[0].shape
    nh, _, dh = w.shape
    assert nh % 2 == 1
    return pl.pallas_call(
        functools.partial(_qkv_kernel, nx),
        out_shape=jax.ShapeDtypeStruct((nh, nx, rb, dh), xs[0].dtype),
        grid=(pl.cdiv(nh, 2),),
        in_specs=[pl.BlockSpec((rb, d), lambda n: (0, 0), pipeline_mode=pl.Buffered(1)) for _ in xs] + [
            pl.BlockSpec((2, d, dh), lambda n: (n, 0, 0)),
            pl.BlockSpec((1, nx, rb, dh), lambda n: (n // (nh // 3), 0, 0, 0)),
            pl.BlockSpec((1, nx, rb, dh), lambda n: (n // (nh // 3), 0, 0, 0))],
        out_specs=pl.BlockSpec((2, nx, rb, dh), lambda n: (n, 0, 0, 0)),
        compiler_params=pltpu.CompilerParams(vmem_limit_bytes=VMEM_LIMIT),
        cost_estimate=pl.CostEstimate(flops=2 * nx * rb * d * nh * dh, transcendentals=0,
                                      bytes_accessed=2 * (nx * rb * d + d * nh * dh + nx * rb * nh * dh)),
        name="qkv",
    )(*xs, w, cos, sin)


def _attn_body(q_ref, k_ref, v_ref, put, sa_ref, sb_ref, ma_ref, mb_ref, l_ref, acc_ref):
    nb, _, b = sa_ref.shape
    dh = acc_ref.shape[1]
    c = dh ** -0.5 * LOG2E
    lanes = [slice(t * dh, (t + 1) * dh) for t in range(b // dh)]
    sc, mx = (sa_ref, sb_ref), (ma_ref, mb_ref)

    def rows(ref, i):
        return ref[pl.ds(pl.multiple_of(i * b, b), b), :]

    def scores(i, j):
        return lax.dot_general(rows(q_ref, i), rows(k_ref, j), (((1,), (1,)), ((), ())),
                               preferred_element_type=jnp.float32)

    def lanemax(m, x):
        for t in lanes:
            m = jnp.maximum(m, x[:, t])
        return m

    def pass1(i, j, slot):
        x = scores(i, j)
        sc[slot][j] = x
        mx[slot][...] = lanemax(mx[slot][...], x)

    def pass1_diag(i, slot):
        x = scores(i, i)
        x = jnp.where(lax.broadcasted_iota(jnp.int32, x.shape, 0) >= lax.broadcasted_iota(jnp.int32, x.shape, 1),
                      x, -jnp.inf)
        sc[slot][i] = x
        m = lanemax(mx[slot][...], x)
        mx[slot][...] = jnp.broadcast_to(jnp.max(m, axis=1, keepdims=True), m.shape)

    def pass2(j, slot):
        m, l, ps = mx[slot][...], l_ref[...], []
        for t in lanes:
            e = jnp.exp2((sc[slot][j, :, t] - m) * c)
            l = l + e
            ps.append(e.astype(v_ref.dtype))
        l_ref[...] = l
        acc_ref[...] += jnp.dot(jnp.concatenate(ps, axis=1), rows(v_ref, j), preferred_element_type=jnp.float32)

    def clear_max(slot):
        mx[slot][...] = jnp.full(mx[slot].shape, -jnp.inf, jnp.float32)

    def block(i, cur):
        l_ref[...] = jnp.zeros_like(l_ref)
        acc_ref[...] = jnp.zeros_like(acc_ref)
        last = isinstance(i, int) and i == nb - 1
        if not last:
            clear_max(1 - cur)

        def inner(j, _):
            if not last:
                pass1(i + 1, j, 1 - cur)
            pass2(j, cur)
            return 0

        lax.fori_loop(0, i + 1, inner, 0)
        if not last:
            pass1_diag(i + 1, 1 - cur)
        put(i, (acc_ref[...] / jnp.sum(l_ref[...], axis=1, keepdims=True)).astype(v_ref.dtype))

    clear_max(0)
    pass1_diag(0, 0)
    for i in range(nb):
        block(i, i % 2)


def _pieces(p):
    near, far = [(-2, 0), (2, 1), (-2, 1), (2, 0)], [(p // 2, 0), (p // 2, 1)]
    return [[(mate, k, i) for mate in mates for k, i in group]
            for mates, group in (((0, 1), [(0, 0), (0, 1)]), ((0,), near), ((1,), near), ((0,), far), ((1,), far))]


def _piece_at(me, p, mate, k, i):
    m = me + 1 - 2 * lax.rem(me, 2) if mate else me
    return 2 * lax.rem(m + k + p, p) + i


def _attn_kernel(p, n, *refs):
    qkv, (o_ref, q_ref, k_ref, v_ref, stage, in_sem, send_sem, recv_sem, own_sem), scratch = (
        refs[:n], refs[n:n + 9], refs[n + 9:])
    hl, t = o_ref.shape[0], o_ref.shape[2]
    rb = qkv[0].shape[2]
    nb, _, b = scratch[0].shape
    per = b // t
    me = lax.axis_index("seq")

    barrier = pltpu.get_barrier_semaphore()
    for d in range(p):
        @pl.when(d != me)
        def _():
            pl.semaphore_signal(barrier, inc=1, device_id={"seq": d}, device_id_type=pl.DeviceIdType.MESH)

    def fetch(h, slot):
        out = []
        for a, group in zip(qkv, _pieces(p)):
            for i, piece in enumerate(group):
                at = pl.ds(pl.multiple_of(_piece_at(me, p, *piece) * rb, rb), rb)
                for j, dst in enumerate((q_ref, k_ref, v_ref)):
                    out.append(pltpu.make_async_copy(a.at[j * hl + h, i], dst.at[slot, at, :],
                                                     in_sem.at[slot, len(out)]))
        return out

    def remote(h, d):
        return pltpu.make_async_remote_copy(
            src_ref=stage.at[h, d], dst_ref=o_ref.at[h, me], send_sem=send_sem.at[h, d], recv_sem=recv_sem.at[h, me],
            device_id={"seq": d}, device_id_type=pl.DeviceIdType.MESH)

    def own(h, d):
        return pltpu.make_async_copy(stage.at[h, d], o_ref.at[h, d], own_sem.at[h])

    def send(h, i):
        for d in range(i * per, (i + 1) * per):
            @pl.when(d != me)
            def _():
                remote(h, d).start()

            @pl.when(d == me)
            def _():
                own(h, d).start()

    for cp in fetch(0, 0):
        cp.start()
    pl.semaphore_wait(barrier, p - 1)

    def head(h, _):
        slot = lax.rem(h, 2)
        for cp in fetch(h, slot):
            cp.wait()

        @pl.when(h + 1 < hl)
        def _():
            for cp in fetch(h + 1, 1 - slot):
                cp.start()

        def put(i, o):
            for u in range(per):
                stage[h, i * per + u] = o[u * t:(u + 1) * t]
            if i > 0:
                send(h, i - 1)
            else:
                @pl.when(h > 0)
                def _():
                    send(h - 1, nb - 1)

        _attn_body(q_ref.at[slot], k_ref.at[slot], v_ref.at[slot], put, *scratch)
        return 0

    lax.fori_loop(0, hl, head, 0)
    send(hl - 1, nb - 1)

    def drain(h, _):
        for d in range(p):
            @pl.when(d != me)
            def _():
                cp = pltpu.make_async_remote_copy(
                    src_ref=stage.at[h, d], dst_ref=o_ref.at[h, d], send_sem=send_sem.at[h, d],
                    recv_sem=recv_sem.at[h, d], device_id={"seq": d}, device_id_type=pl.DeviceIdType.MESH)
                cp.wait_send()
                cp.wait_recv()

            @pl.when(d == me)
            def _():
                own(h, d).wait()
        return 0

    lax.fori_loop(0, hl, drain, 0)


def _attn(qkv, p, b=1024):
    n = len(qkv)
    nh, _, rb, dh = qkv[0].shape
    nx = sum(a.shape[1] for a in qkv)
    s, hl, dt = nx * rb, nh // 3, qkv[0].dtype
    f32 = jnp.float32
    return pl.pallas_call(
        functools.partial(_attn_kernel, p, n),
        out_shape=jax.ShapeDtypeStruct((hl, p, s // p, dh), dt),
        in_specs=[pl.BlockSpec(memory_space=pl.ANY)] * n,
        out_specs=pl.BlockSpec(memory_space=pl.ANY),
        scratch_shapes=[pltpu.VMEM((2, s, dh), dt)] * 3 + [
            pltpu.VMEM((hl, p, s // p, dh), dt), pltpu.SemaphoreType.DMA((2, 3 * nx)),
            pltpu.SemaphoreType.DMA((hl, p)), pltpu.SemaphoreType.DMA((hl, p)), pltpu.SemaphoreType.DMA((hl,)),
            pltpu.VMEM((s // b, b, b), f32), pltpu.VMEM((s // b, b, b), f32), pltpu.VMEM((b, dh), f32),
            pltpu.VMEM((b, dh), f32), pltpu.VMEM((b, dh), f32), pltpu.VMEM((b, dh), f32)],
        compiler_params=pltpu.CompilerParams(vmem_limit_bytes=VMEM_LIMIT, collective_id=0, has_side_effects=True),
        cost_estimate=pl.CostEstimate(flops=2 * 2 * s * s * dh * hl, transcendentals=hl * s * s // 2,
                                      bytes_accessed=2 * 4 * s * dh * hl),
        name="attn",
    )(*qkv)


def _out_kernel(o_ref, w_ref, x_ref, y_ref):
    acc = x_ref[...].astype(jnp.float32)
    p, nc, dh, cols = w_ref.shape
    for c in range(nc):
        o = jnp.concatenate([o_ref[c, s] for s in range(p)], axis=1)
        acc += jnp.dot(o, w_ref[:, c].reshape(p * dh, cols), preferred_element_type=jnp.float32)
    y_ref[...] = acc.astype(y_ref.dtype)


def _out(o, wo, x, cols=256):
    nc, p, t, dh = o.shape
    d = x.shape[1]
    return pl.pallas_call(
        _out_kernel,
        out_shape=jax.ShapeDtypeStruct(x.shape, x.dtype),
        grid=(d // cols,),
        in_specs=[pl.BlockSpec((nc, p, t, dh), lambda n: (0, 0, 0, 0), pipeline_mode=pl.Buffered(1)),
                  pl.BlockSpec((p, nc, dh, cols), lambda n: (0, 0, 0, n)),
                  pl.BlockSpec((t, cols), lambda n: (0, n))],
        out_specs=pl.BlockSpec((t, cols), lambda n: (0, n)),
        compiler_params=pltpu.CompilerParams(vmem_limit_bytes=VMEM_LIMIT),
        cost_estimate=pl.CostEstimate(flops=2 * t * d * p * nc * dh, transcendentals=0,
                                      bytes_accessed=2 * (p * nc * dh * d + 3 * t * d)),
        name="outproj",
    )(o, wo.reshape(p, nc, dh, d), x)


def _shift(a, p, k):
    return lax.ppermute(a, "seq", [(i, (i + k) % p) for i in range(p)])


def _partner(a, p):
    return lax.ppermute(a, "seq", [(i, i ^ 1) for i in range(p)])


def solution(mesh):
    p = mesh.shape["seq"]
    rows = P(("data", "seq"), None)

    def local(x, g, wqkv, wo):
        t, d = x.shape
        _, _, h, dh = wqkv.shape
        hl = h // p
        me = lax.axis_index("seq")
        rb = t // 2

        def norm(x):
            xf = x.astype(jnp.float32)
            return (xf * lax.rsqrt(jnp.mean(xf * xf, axis=-1, keepdims=True) + 1e-5) * g).astype(jnp.bfloat16)

        xa, xb = norm(x[:rb]), norm(x[rb:])
        left_a, right_b = _shift(xa, p, 2), _shift(xb, p, -2)
        left_b, right_a = _shift(xb, p, 2), _shift(xa, p, -2)

        w = lax.dynamic_slice_in_dim(wqkv, hl * me, hl, 2).transpose(1, 2, 0, 3).reshape(3 * hl, d, dh)
        half = dh // 2
        inv = 10000.0 ** (-jnp.arange(half, dtype=jnp.float32) * 2.0 / dh)

        def tables(group):
            idx = jnp.stack([_piece_at(me, p, *piece) for piece in group])
            ang = (idx[:, None] * rb + jnp.arange(rb)).astype(jnp.float32)[:, :, None] * inv
            cos, sin = jnp.cos(ang), jnp.sin(ang)
            cos, sin = jnp.concatenate([cos, cos], 2), jnp.concatenate([-sin, sin], 2)
            return jnp.stack([cos, jnp.ones_like(cos)]), jnp.stack([sin, jnp.zeros_like(sin)])

        def mates(xs):
            return [_partner(a, p) for a in xs]

        def after(done, *later):
            return lax.optimization_barrier((done, *later))

        tabs = [tables(group) for group in _pieces(p)]
        near = [left_a, right_b, left_b, right_a]
        own = _qkv([xa, xb] + mates([xa, xb]), w, *tabs[0])
        own, near, tabs = after(own, near, tabs)
        far = [_shift(near[0], p, 2), _shift(near[1], p, -2)]
        near_m = mates(near)
        q_near = _qkv(near, w, *tabs[1])
        q_near, near_m = after(q_near, near_m)
        q_near_m = _qkv(near_m, w, *tabs[2])
        q_near_m, far = after(q_near_m, far)
        far_m = mates(far)
        q_far = _qkv(far, w, *tabs[3])
        q_far, far_m = after(q_far, far_m)
        qkv = [own, q_near, q_near_m, q_far, _qkv(far_m, w, *tabs[4])]

        return _out(_attn(qkv, p), wo, x)

    return jax.shard_map(local, mesh=mesh,
                         in_specs=(rows, P(None), P(None, None, None, None), P(None, None, None)),
                         out_specs=rows, check_vma=False)
```

```python
import functools

import jax
import jax.numpy as jnp
from jax import lax
from jax.experimental import pallas as pl
from jax.experimental.pallas import tpu as pltpu
from jax.sharding import PartitionSpec as P


LOG2E = 1.4426950408889634
VMEM_LIMIT = 60 * 1024 * 1024


def _qkv_kernel(nx, nrope, *refs):
    xs, w_ref, cos_ref, sin_ref, out_ref = refs[:nx], *refs[nx:]
    n, steps = pl.program_id(0), pl.num_programs(0)
    nh, _, _, dh = out_ref.shape
    rope = n < nrope

    @pl.when(n < steps - 1)
    def _():
        w = jnp.concatenate([w_ref[h] for h in range(nh)], axis=1)
        for i in range(nx):
            acc = jnp.dot(xs[i][...], w, preferred_element_type=jnp.float32)
            cos, sin = jnp.where(rope, cos_ref[i], 1.0), jnp.where(rope, sin_ref[i], 0.0)
            for h in range(nh):
                a = acc[:, h * dh:(h + 1) * dh]
                rot = pltpu.roll(a, dh // 2, 1)
                out_ref[h, i] = (a * cos + rot * sin).astype(out_ref.dtype)

    @pl.when(n == steps - 1)
    def _():
        for i in range(nx):
            out_ref[0, i] = jnp.dot(xs[i][...], w_ref[0], preferred_element_type=jnp.float32).astype(out_ref.dtype)


def _qkv(xs, w, cos, sin, at):
    nx = len(xs)
    rb, d = xs[0].shape
    nh, _, dh = w.shape
    assert nh % 2 == 1
    return pl.pallas_call(
        functools.partial(_qkv_kernel, nx, nh // 3),
        out_shape=jax.ShapeDtypeStruct((nh, nx, rb, dh), xs[0].dtype),
        grid=(pl.cdiv(nh, 2),),
        in_specs=[pl.BlockSpec((rb, d), lambda n: (0, 0), pipeline_mode=pl.Buffered(1)) for _ in xs] + [
            pl.BlockSpec((2, d, dh), lambda n: (n, 0, 0)),
            pl.BlockSpec((nx, rb, dh), lambda n: (at // nx, 0, 0), pipeline_mode=pl.Buffered(1)),
            pl.BlockSpec((nx, rb, dh), lambda n: (at // nx, 0, 0), pipeline_mode=pl.Buffered(1))],
        out_specs=pl.BlockSpec((2, nx, rb, dh), lambda n: (n, 0, 0, 0)),
        compiler_params=pltpu.CompilerParams(vmem_limit_bytes=VMEM_LIMIT),
        name="qkv",
    )(*xs, w, cos, sin)


def _attn_body(q_ref, k_ref, v_ref, put, sa_ref, sb_ref, ma_ref, mb_ref, l_ref, acc_ref):
    nb, _, b = sa_ref.shape
    dh = acc_ref.shape[1]
    c = dh ** -0.5 * LOG2E
    lanes = [slice(t * dh, (t + 1) * dh) for t in range(b // dh)]
    sc, mx = (sa_ref, sb_ref), (ma_ref, mb_ref)

    def rows(ref, i):
        return ref[pl.ds(pl.multiple_of(i * b, b), b), :]

    def scores(i, j):
        return lax.dot_general(rows(q_ref, i), rows(k_ref, j), (((1,), (1,)), ((), ())),
                               preferred_element_type=jnp.float32)

    def lanemax(m, x):
        for t in lanes:
            m = jnp.maximum(m, x[:, t])
        return m

    def pass1(i, j, slot):
        x = scores(i, j)
        sc[slot][j] = x
        mx[slot][...] = lanemax(mx[slot][...], x)

    hb = b // 2

    def pass1_diag(i, slot):
        for u in range(2):
            n = (u + 1) * hb
            at = pl.ds(pl.multiple_of(i * b + u * hb, hb), hb)
            k = k_ref[pl.ds(pl.multiple_of(i * b, b), n), :]
            x = lax.dot_general(q_ref[at, :], k, (((1,), (1,)), ((), ())), preferred_element_type=jnp.float32)
            row = lax.broadcasted_iota(jnp.int32, (hb, hb), 0)
            tail = jnp.where(row >= lax.broadcasted_iota(jnp.int32, (hb, hb), 1), x[:, u * hb:], -jnp.inf)
            part = slice(u * hb, n)
            m = mx[slot][part]
            if u:
                sc[slot][i, part, :hb] = x[:, :hb]
                for t in range(hb // dh):
                    m = jnp.maximum(m, x[:, t * dh:(t + 1) * dh])
            sc[slot][i, part, part] = tail
            for t in range(hb // dh):
                m = jnp.maximum(m, tail[:, t * dh:(t + 1) * dh])
            mx[slot][part] = jnp.broadcast_to(jnp.max(m, axis=1, keepdims=True), m.shape)

    def pass2_diag(i, slot):
        for u in range(2):
            part = slice(u * hb, (u + 1) * hb)
            m, l, ps = mx[slot][part], l_ref[part], []
            for t in range((u + 1) * hb // dh):
                e = jnp.exp2((sc[slot][i, part, t * dh:(t + 1) * dh] - m) * c)
                l = l + e
                ps.append(e.astype(v_ref.dtype))
            l_ref[part] = l
            v = v_ref[pl.ds(pl.multiple_of(i * b, b), (u + 1) * hb), :]
            acc_ref[part] += jnp.dot(jnp.concatenate(ps, axis=1), v, preferred_element_type=jnp.float32)

    def pass2(j, slot):
        m, l, ps = mx[slot][...], l_ref[...], []
        for t in lanes:
            e = jnp.exp2((sc[slot][j, :, t] - m) * c)
            l = l + e
            ps.append(e.astype(v_ref.dtype))
        l_ref[...] = l
        acc_ref[...] += jnp.dot(jnp.concatenate(ps, axis=1), rows(v_ref, j), preferred_element_type=jnp.float32)

    def clear_max(slot):
        mx[slot][...] = jnp.full(mx[slot].shape, -jnp.inf, jnp.float32)

    def block(i, cur):
        l_ref[...] = jnp.zeros_like(l_ref)
        acc_ref[...] = jnp.zeros_like(acc_ref)
        last = isinstance(i, int) and i == nb - 1
        if not last:
            clear_max(1 - cur)

        def inner(j, _):
            if not last:
                pass1(i + 1, j, 1 - cur)
            pass2(j, cur)
            return 0

        lax.fori_loop(0, i, inner, 0)
        if not last:
            pass1(i + 1, i, 1 - cur)
        pass2_diag(i, cur)
        if not last:
            pass1_diag(i + 1, 1 - cur)
        put(i, (acc_ref[...] / jnp.sum(l_ref[...], axis=1, keepdims=True)).astype(v_ref.dtype))

    clear_max(0)
    pass1_diag(0, 0)
    for i in range(nb):
        block(i, i % 2)


def _pieces(p):
    own, first, second = [(0, 0), (0, 1)], [(-2, 0), (2, 1)], [(-2, 1), (2, 0)]
    far = [(p // 2, 0), (p // 2, 1)]
    return [[(mate, k, i) for mate in mates for k, i in group]
            for mates, group in (((0, 1), own), ((0, 1), first), ((0,), second), ((1,), second), ((0,), far), ((1,), far))]


def _piece_at(me, p, mate, k, i):
    m = me + 1 - 2 * lax.rem(me, 2) if mate else me
    return 2 * lax.rem(m + k + p, p) + i


def _attn_kernel(p, n, *refs):
    qkv, (o_ref, q_ref, k_ref, v_ref, stage, in_sem, send_sem, recv_sem, own_sem), scratch = (
        refs[:n], refs[n:n + 9], refs[n + 9:])
    hl, t = o_ref.shape[0], o_ref.shape[2]
    rb = qkv[0].shape[2]
    nb, _, b = scratch[0].shape
    per = b // t
    me = lax.axis_index("seq")

    barrier = pltpu.get_barrier_semaphore()
    for d in range(p):
        @pl.when(d != me)
        def _():
            pl.semaphore_signal(barrier, inc=1, device_id={"seq": d}, device_id_type=pl.DeviceIdType.MESH)

    def fetch(h, slot):
        out = []
        for a, group in zip(qkv, _pieces(p)):
            for i, piece in enumerate(group):
                at = pl.ds(pl.multiple_of(_piece_at(me, p, *piece) * rb, rb), rb)
                for j, dst in enumerate((q_ref, k_ref, v_ref)):
                    out.append(pltpu.make_async_copy(a.at[j * hl + h, i], dst.at[slot, at, :],
                                                     in_sem.at[slot, len(out)]))
        return out

    def remote(h, d):
        return pltpu.make_async_remote_copy(
            src_ref=stage.at[h, d], dst_ref=o_ref.at[h, me], send_sem=send_sem.at[h, d], recv_sem=recv_sem.at[h, me],
            device_id={"seq": d}, device_id_type=pl.DeviceIdType.MESH)

    def own(h, d):
        return pltpu.make_async_copy(stage.at[h, d], o_ref.at[h, d], own_sem.at[h])

    def send(h, i):
        for d in range(i * per, (i + 1) * per):
            @pl.when(d != me)
            def _():
                remote(h, d).start()

            @pl.when(d == me)
            def _():
                own(h, d).start()

    for cp in fetch(0, 0):
        cp.start()
    pl.semaphore_wait(barrier, p - 1)

    def head(h, _):
        slot = lax.rem(h, 2)
        for cp in fetch(h, slot):
            cp.wait()

        @pl.when(h + 1 < hl)
        def _():
            for cp in fetch(h + 1, 1 - slot):
                cp.start()

        def put(i, o):
            for u in range(per):
                stage[h, i * per + u] = o[u * t:(u + 1) * t]
            if i > 0:
                send(h, i - 1)
            else:
                @pl.when(h > 0)
                def _():
                    send(h - 1, nb - 1)

        _attn_body(q_ref.at[slot], k_ref.at[slot], v_ref.at[slot], put, *scratch)
        return 0

    lax.fori_loop(0, hl, head, 0)
    send(hl - 1, nb - 1)

    def drain(h, _):
        for d in range(p):
            @pl.when(d != me)
            def _():
                cp = pltpu.make_async_remote_copy(
                    src_ref=stage.at[h, d], dst_ref=o_ref.at[h, d], send_sem=send_sem.at[h, d],
                    recv_sem=recv_sem.at[h, d], device_id={"seq": d}, device_id_type=pl.DeviceIdType.MESH)
                cp.wait_send()
                cp.wait_recv()

            @pl.when(d == me)
            def _():
                own(h, d).wait()
        return 0

    lax.fori_loop(0, hl, drain, 0)


def _attn(qkv, p, b=1024):
    n = len(qkv)
    nh, _, rb, dh = qkv[0].shape
    nx = sum(a.shape[1] for a in qkv)
    s, hl, dt = nx * rb, nh // 3, qkv[0].dtype
    f32 = jnp.float32
    return pl.pallas_call(
        functools.partial(_attn_kernel, p, n),
        out_shape=jax.ShapeDtypeStruct((hl, p, s // p, dh), dt),
        in_specs=[pl.BlockSpec(memory_space=pl.ANY)] * n,
        out_specs=pl.BlockSpec(memory_space=pl.ANY),
        scratch_shapes=[pltpu.VMEM((2, s, dh), dt)] * 3 + [
            pltpu.VMEM((hl, p, s // p, dh), dt), pltpu.SemaphoreType.DMA((2, 3 * nx)),
            pltpu.SemaphoreType.DMA((hl, p)), pltpu.SemaphoreType.DMA((hl, p)), pltpu.SemaphoreType.DMA((hl,)),
            pltpu.VMEM((s // b, b, b), f32), pltpu.VMEM((s // b, b, b), f32), pltpu.VMEM((b, dh), f32),
            pltpu.VMEM((b, dh), f32), pltpu.VMEM((b, dh), f32), pltpu.VMEM((b, dh), f32)],
        compiler_params=pltpu.CompilerParams(vmem_limit_bytes=VMEM_LIMIT, collective_id=0, has_side_effects=True),
        cost_estimate=pl.CostEstimate(flops=2 * 2 * s * s * dh * hl, transcendentals=hl * s * s // 2,
                                      bytes_accessed=2 * 4 * s * dh * hl),
        name="attn",
    )(*qkv)


def _out_kernel(o_ref, w_ref, x_ref, y_ref):
    acc = x_ref[...].astype(jnp.float32)
    p, nc, dh, cols = w_ref.shape
    for c in range(nc):
        o = jnp.concatenate([o_ref[c, s] for s in range(p)], axis=1)
        acc += jnp.dot(o, w_ref[:, c].reshape(p * dh, cols), preferred_element_type=jnp.float32)
    y_ref[...] = acc.astype(y_ref.dtype)


def _out(o, wo, x, cols=512):
    nc, p, t, dh = o.shape
    d = x.shape[1]
    return pl.pallas_call(
        _out_kernel,
        out_shape=jax.ShapeDtypeStruct(x.shape, x.dtype),
        grid=(d // cols,),
        in_specs=[pl.BlockSpec((nc, p, t, dh), lambda n: (0, 0, 0, 0), pipeline_mode=pl.Buffered(1)),
                  pl.BlockSpec((p, nc, dh, cols), lambda n: (0, 0, 0, n)),
                  pl.BlockSpec((t, cols), lambda n: (0, n))],
        out_specs=pl.BlockSpec((t, cols), lambda n: (0, n)),
        compiler_params=pltpu.CompilerParams(vmem_limit_bytes=VMEM_LIMIT),
        cost_estimate=pl.CostEstimate(flops=2 * t * d * p * nc * dh, transcendentals=0,
                                      bytes_accessed=2 * (p * nc * dh * d + 3 * t * d)),
        name="outproj",
    )(o, wo.reshape(p, nc, dh, d), x)


def _shift(a, p, k):
    return lax.ppermute(a, "seq", [(i, (i + k) % p) for i in range(p)])


def _partner(a, p):
    return lax.ppermute(a, "seq", [(i, i ^ 1) for i in range(p)])


def solution(mesh):
    p = mesh.shape["seq"]
    rows = P(("data", "seq"), None)

    def local(x, g, wqkv, wo):
        t, d = x.shape
        _, _, h, dh = wqkv.shape
        hl = h // p
        me = lax.axis_index("seq")
        rb = t // 2

        def norm(x):
            xf = x.astype(jnp.float32)
            return (xf * lax.rsqrt(jnp.mean(xf * xf, axis=-1, keepdims=True) + 1e-5) * g).astype(jnp.bfloat16)

        def mates(xs):
            return [_partner(a, p) for a in xs]

        def after(done, later):
            return lax.optimization_barrier((done, later))

        xa, xb = norm(x[:rb]), norm(x[rb:])
        first = [_shift(xa, p, 2), _shift(xb, p, -2)]
        mate = mates([xa, xb])

        w = lax.dynamic_slice_in_dim(wqkv, hl * me, hl, 2).transpose(1, 2, 0, 3).reshape(3 * hl, d, dh)
        half = dh // 2
        inv = 10000.0 ** (-(jnp.arange(dh) % half).astype(jnp.float32) * 2.0 / dh)
        sign = jnp.where(jnp.arange(dh) < half, -1.0, 1.0)
        pos = jnp.stack([_piece_at(me, p, *piece) for group in _pieces(p) for piece in group])[:, None] * rb + jnp.arange(rb)
        ang = pos.astype(jnp.float32)[:, :, None] * inv
        cos, sin = jnp.cos(ang), jnp.sin(ang) * sign

        w, (xa, xb, *first) = after(w, (xa, xb, *first))
        second = [_shift(xb, p, 2), _shift(xa, p, -2)]
        first_m = mates(first)
        own = _qkv([xa, xb] + mate, w, cos, sin, 0)
        own, onward = after(own, first)
        far = [_shift(onward[0], p, 2), _shift(onward[1], p, -2)]
        q_first = _qkv(first + first_m, w, cos, sin, 4)
        q_first, second = after(q_first, second)
        second_m = mates(second)
        q_second = _qkv(second, w, cos, sin, 8)
        q_second, second_m = after(q_second, second_m)
        q_second_m = _qkv(second_m, w, cos, sin, 10)
        q_second_m, far = after(q_second_m, far)
        far_m = mates(far)
        q_far = _qkv(far, w, cos, sin, 12)
        q_far, far_m = after(q_far, far_m)
        qkv = [own, q_first, q_second, q_second_m, q_far, _qkv(far_m, w, cos, sin, 14)]

        return _out(_attn(qkv, p), wo, x)

    return jax.shard_map(local, mesh=mesh,
                         in_specs=(rows, P(None), P(None, None, None, None), P(None, None, None)),
                         out_specs=rows, check_vma=False)
```
